32 devices in a mesh: dp: 8 (over y, x, core), tensor: 4 (over z).
Axes of the slice: x: 2, y: 2, z: 4, core: 2. Of those that a mesh axis runs over, the one named last changes fastest.
Arguments:
- resid_in: float32 [8192, 2048], P(('dp', 'tensor')), may hold values from -6 to 6
- lengths: int32 [8], P('dp'), may hold values from 256 to 1024, as said below
- qkv_weight: bfloat16 [2048, 3072], P('dp', 'tensor'), may hold values from -0.125 to 0.125
- out_weight: bfloat16 [2048, 2048], P('tensor', 'dp'), may hold values from -2 to 2
- gate_weight: bfloat16 [2048, 8192], P('dp', 'tensor'), may hold values from -0.125 to 0.125
- up_weight: bfloat16 [2048, 8192], P('dp', 'tensor'), may hold values from -0.125 to 0.125
- down_weight: bfloat16 [8192, 2048], P('tensor', 'dp'), may hold values from -0.0625 to 0.0625
- attn_gain: bfloat16 [2048], P('dp'), may hold values from 0.25 to 1.75
- mlp_gain: bfloat16 [2048], P('dp'), may hold values from 0.25 to 1.75
- query_gain: float32 [64], replicated, may hold values from 0.5 to 2
- key_gain: float32 [64], replicated, may hold values from 0.5 to 2
- out_grad: float32 [8192, 2048], P(('dp', 'tensor')), may hold values from -6 to 6
Outputs:
- block_out: float32 [8192, 2048], P(('dp', 'tensor'))
- resid_grad: float32 [8192, 2048], P(('dp', 'tensor'))
- qkv_grad: float32 [2048, 3072], P('dp', 'tensor')
- outproj_grad: float32 [2048, 2048], P('tensor', 'dp')
- gate_grad: float32 [2048, 8192], P('dp', 'tensor')
- up_grad: float32 [2048, 8192], P('dp', 'tensor')
- down_grad: float32 [8192, 2048], P('tensor', 'dp')
- attngain_grad: float32 [2048], P('dp')
- mlpgain_grad: float32 [2048], P('dp')
- querygain_grad: float32 [64], replicated
- keygain_grad: float32 [64], replicated
The draws below stay inside these ranges and needn't reach their ends.
Inputs may be any that keep to these rules, and one draw needn't show every extreme that they name: `lengths`: some batch holds a single sequence of all 1024 slots, and some batch begins with a sequence of exactly 256 slots.
All inputs are finite; a program needn't handle non-finite values.
Results may differ from the reference program's by a relative error of at most 0.024.
Values may be sent and summed in bfloat16 or wider, within the bound.
A program may use at most 256 MiB of HBM per device.

```python
import math
import jax
import jax.numpy as jnp
from jax import lax

D = 2048
HEADS = 32
KV_HEADS = 8
HEAD_DIM = 64
FF = 8192
GROUP_TOK = 1024
MIN_LEN = 256
ATT = 2048
QKV = 3072
TOKENS = 8192
N_DP = 8
N_TENSOR = 4


def draw_lengths(key, part):
    drawn = jax.random.randint(jax.random.fold_in(key, 11), (N_DP,), MIN_LEN, GROUP_TOK + 1, dtype=jnp.int32)
    order = jax.random.permutation(jax.random.fold_in(key, 12), N_DP)
    drawn = drawn.at[order[0]].set(GROUP_TOK)
    drawn = drawn.at[order[1]].set(MIN_LEN)
    return drawn


def strengthened(result, stream_key, source, target, shards_of, factor):
    def block_of(dim):
        return (jnp.arange(result.shape[dim]) // (result.shape[dim] // shards_of)).reshape((-1,) + (1,) * (result.ndim - 1 - dim))

    first = jax.random.permutation(stream_key, shards_of)[block_of(target)]
    far = (block_of(target) + shards_of // 2) % shards_of
    return jnp.where((block_of(source) == first) | (block_of(source) == far), factor * result, result)


def shard_levels(key, shape, split, smallest, top_value):
    level = 1.0
    for dim, parts in split:
        steps = jax.random.uniform(jax.random.fold_in(jax.random.fold_in(key, 6), dim), (parts,), jnp.float32, smallest / len(split), top_value / len(split))
        level = level * jnp.repeat(jnp.exp(steps), shape[dim] // parts).reshape((-1,) + (1,) * (len(shape) - 1 - dim))
    return level


def bell_draw(own_key, dims, scale, bound, split=(), kind=jnp.bfloat16):
    array = scale * jax.random.normal(own_key, dims, jnp.float32)
    if split:
        array = array * shard_levels(own_key, dims, split, -0.22, 0.18)
    return jnp.clip(array, -bound, bound).astype(kind)


def gaussian_with(key, dims, spread, most, shards, heavy, kind=jnp.bfloat16):
    values = spread * jax.random.normal(key, dims, jnp.float32)
    if shards:
        values = values * shard_levels(key, dims, shards, -0.22, 0.18)
    return jnp.clip(strengthened(values, jax.random.fold_in(key, 3), *heavy), -most, most).astype(kind)


def setup_inputs(seed: int = 0) -> dict:
    arg_keys = jax.random.split(jax.random.key(seed), 13)
    resid_in = bell_draw(arg_keys[0], (TOKENS, D), 1.0, 6.0, ((0, 32),), jnp.float32)
    lengths = draw_lengths(jax.random.fold_in(arg_keys[12], 71), 0)
    qkv_weight = bell_draw(arg_keys[2], (D, QKV), D ** -0.5, 0.125, ((0, 8), (1, 4)))
    out_weight = bell_draw(arg_keys[3], (ATT, D), (max(D // 256, 4)) ** -0.5, 2.0, ((0, 4), (1, 8)))
    gate_weight = bell_draw(arg_keys[4], (D, FF), D ** -0.5, 0.125, ((0, 8), (1, 4)))
    up_weight = bell_draw(arg_keys[5], (D, FF), D ** -0.5, 0.125, ((0, 8), (1, 4)))
    down_weight = bell_draw(arg_keys[6], (FF, D), FF ** -0.5, 0.0625, ((0, 4), (1, 8)))
    attn_gain = jnp.clip(1.0 + 0.15 * jax.random.normal(arg_keys[7], (D,), jnp.float32), 0.25, 1.75).astype(jnp.bfloat16)
    mlp_gain = jnp.clip(1.0 + 0.15 * jax.random.normal(arg_keys[8], (D,), jnp.float32), 0.25, 1.75).astype(jnp.bfloat16)
    query_gain = jnp.clip(jnp.exp(jax.random.uniform(arg_keys[9], (HEAD_DIM,), jnp.float32, math.log(0.5), math.log(2.0))), 0.5, 2.0)
    key_gain = jnp.clip(jnp.exp(jax.random.uniform(arg_keys[10], (HEAD_DIM,), jnp.float32, math.log(0.5), math.log(2.0))), 0.5, 2.0)
    out_grad = gaussian_with(arg_keys[11], (TOKENS, D), 1.0, 6.0, ((0, 32),), (0, 1, 32, 2.75), jnp.float32)
    return {"resid_in": resid_in, "lengths": lengths, "qkv_weight": qkv_weight, "out_weight": out_weight, "gate_weight": gate_weight, "up_weight": up_weight, "down_weight": down_weight, "attn_gain": attn_gain, "mlp_gain": mlp_gain, "query_gain": query_gain, "key_gain": key_gain, "out_grad": out_grad}


EPS = 1e-05
ROPE_BASE = 1000000.0

def inv_rms(value):
    return lax.rsqrt(lax.optimization_barrier(jnp.mean(value * value, axis=-1, keepdims=True)) + EPS)

def norm_back(grad_unit, unit, inverse):
    return inverse * (grad_unit - unit * lax.optimization_barrier(jnp.mean(grad_unit * unit, axis=-1, keepdims=True)))

def rope_tables(position, head_size):
    half = head_size // 2
    freq = ROPE_BASE ** (-(2.0 * jnp.arange(half, dtype=jnp.float32)) / head_size)
    angle = position.astype(jnp.float32)[:, None] * freq[None, :]
    return (jnp.cos(angle), jnp.sin(angle))

def widen(table, ndim):
    return table.reshape(table.shape[:1] + (1,) * (ndim - 2) + table.shape[1:])

def rotate(value, cosine, sine):
    half = value.shape[-1] // 2
    first, second = (value[..., :half], value[..., half:])
    cosine, sine = (widen(cosine, value.ndim), widen(sine, value.ndim))
    return jnp.concatenate([first * cosine - second * sine, second * cosine + first * sine], axis=-1)

def rotate_back(grad, cosine, sine):
    half = grad.shape[-1] // 2
    first, second = (grad[..., :half], grad[..., half:])
    cosine, sine = (widen(cosine, grad.ndim), widen(sine, grad.ndim))
    return jnp.concatenate([first * cosine + second * sine, second * cosine - first * sine], axis=-1)

def visible(start, height, live):
    query_idx = start + jnp.arange(height, dtype=jnp.int32)
    key_idx = jnp.arange(live.shape[0], dtype=jnp.int32)
    query_live = lax.dynamic_slice_in_dim(live, start, height, 0)
    return (key_idx[None, :] <= query_idx[:, None]) & (query_live[:, None] == live[None, :])

def split_heads(packed_all, query_gain, key_gain, cosine, sine):
    height = packed_all.shape[0]
    group = HEADS // KV_HEADS
    packed = packed_all.reshape(height, -1, (group + 2) * HEAD_DIM)
    query = packed[:, :, :group * HEAD_DIM].reshape(height, packed.shape[1], group, HEAD_DIM)
    keys = packed[:, :, group * HEAD_DIM:(group + 1) * HEAD_DIM]
    values = packed[:, :, (group + 1) * HEAD_DIM:]
    q_inv = inv_rms(query)
    q_unit = query * q_inv
    k_inv = inv_rms(keys)
    k_unit = keys * k_inv
    q_rot = rotate(q_unit * query_gain, cosine, sine).astype(jnp.bfloat16)
    k_rot = rotate(k_unit * key_gain, cosine, sine).astype(jnp.bfloat16)
    return (q_rot, k_rot, values.astype(jnp.bfloat16), q_unit, k_unit, q_inv, k_inv)

def attend_forward(q_rot, k_rot, v_b, live):
    height = q_rot.shape[0]
    block = min(512, height)
    scale = HEAD_DIM ** (-0.5)
    keys32 = k_rot.astype(jnp.float32)
    vals32 = v_b.astype(jnp.float32)

    def one_block(start):
        q_part = lax.dynamic_slice_in_dim(q_rot, start, block, 0).astype(jnp.float32)
        scores = jnp.einsum('qgjd,kgd->gjqk', q_part, keys32) * scale
        scores = jnp.where(visible(start, block, live), scores, -jnp.inf)
        top = lax.optimization_barrier(jnp.max(scores, axis=-1, keepdims=True))
        expo = jnp.exp(scores - top)
        total = lax.optimization_barrier(jnp.sum(expo, axis=-1, keepdims=True))
        probs_b = (expo / total).astype(jnp.bfloat16)
        out = jnp.einsum('gjqk,kgd->qgjd', probs_b.astype(jnp.float32), vals32)
        return (out.astype(jnp.bfloat16), (top + jnp.log(total))[..., 0])
    starts = jnp.arange(height // block, dtype=jnp.int32) * block
    out_blocks, lse_blocks = lax.map(one_block, starts)
    return (out_blocks.reshape(q_rot.shape), lse_blocks, starts)

def attend_backward(q_rot, k_rot, v_b, live, lse_blocks, starts, grad_attn):
    height = q_rot.shape[0]
    block = min(512, height)
    scale = HEAD_DIM ** (-0.5)
    keys32 = k_rot.astype(jnp.float32)
    vals32 = v_b.astype(jnp.float32)

    def one_block(carry, item):
        k_acc, v_acc = carry
        start, lse_part = item
        q_part = lax.dynamic_slice_in_dim(q_rot, start, block, 0).astype(jnp.float32)
        g_part = lax.dynamic_slice_in_dim(grad_attn, start, block, 0).astype(jnp.float32)
        scores = jnp.einsum('qgjd,kgd->gjqk', q_part, keys32) * scale
        scores = jnp.where(visible(start, block, live), scores, -jnp.inf)
        probs = jnp.exp(scores - lse_part[..., None])
        d_probs = jnp.einsum('qgjd,kgd->gjqk', g_part, vals32)
        delta = lax.optimization_barrier(jnp.sum(probs * d_probs, axis=-1, keepdims=True))
        d_scores = (probs * (d_probs - delta)).astype(jnp.bfloat16).astype(jnp.float32)
        probs_b = probs.astype(jnp.bfloat16).astype(jnp.float32)
        q_grad = jnp.einsum('gjqk,kgd->qgjd', d_scores, keys32) * scale
        k_acc = k_acc + jnp.einsum('gjqk,qgjd->kgd', d_scores, q_part) * scale
        v_acc = v_acc + jnp.einsum('gjqk,qgjd->kgd', probs_b, g_part)
        return ((k_acc, v_acc), q_grad)
    zeros = jnp.zeros(k_rot.shape, jnp.float32)
    (k_grad, v_grad), q_blocks = lax.scan(one_block, (zeros, zeros), (starts, lse_blocks))
    return (q_blocks.reshape(q_rot.shape), k_grad, v_grad)

def merge_back(q_grad, k_grad, v_grad, q_unit, k_unit, q_inv, k_inv, query_gain, key_gain, cosine, sine):
    q_turn = rotate_back(q_grad, cosine, sine)
    k_turn = rotate_back(k_grad, cosine, sine)
    qgain_part = lax.optimization_barrier(jnp.sum(q_turn * q_unit, axis=(0, 1, 2)))
    kgain_part = lax.optimization_barrier(jnp.sum(k_turn * k_unit, axis=(0, 1)))
    q_pre = norm_back(q_turn * query_gain, q_unit, q_inv)
    k_pre = norm_back(k_turn * key_gain, k_unit, k_inv)
    height = q_pre.shape[0]
    packed = jnp.concatenate([q_pre.reshape(height, q_pre.shape[1], -1), k_pre, v_grad], axis=2)
    return (packed.reshape(height, -1).astype(jnp.bfloat16), qgain_part, kgain_part)

def block_sum(pairs):
    total = None
    for left, right in pairs:
        lhs = left.astype(jnp.float32).reshape(left.shape[0], N_TENSOR, -1)
        rhs = right.astype(jnp.float32).reshape(N_TENSOR, -1, right.shape[1])
        term = jnp.einsum('gtf,tfd->tgd', lhs, rhs)
        total = term if total is None else total + term
    rounded = lax.optimization_barrier(total.astype(jnp.bfloat16))
    return lax.optimization_barrier(jnp.sum(rounded.astype(jnp.float32), axis=0))

def reference(resid_in, lengths, qkv_weight, out_weight, gate_weight, up_weight, down_weight, attn_gain, mlp_gain, query_gain, key_gain, out_grad):
    f32 = jnp.float32
    bf16 = jnp.bfloat16
    groups = lengths.shape[0]
    width = resid_in.shape[1]
    group_rows = resid_in.shape[0] // groups
    gain_a = attn_gain.astype(f32)
    gain_m = mlp_gain.astype(f32)

    def one_group(carry, item):
        resid, seq_length, grad_out = item
        slots = jnp.arange(group_rows, dtype=jnp.int32)
        live = slots < seq_length
        cosine, sine = rope_tables(jnp.where(live, slots, slots - seq_length), HEAD_DIM)
        inv_a = inv_rms(resid)
        unit_a = resid * inv_a
        normed_a = (unit_a * gain_a).astype(bf16)
        packed = jnp.dot(normed_a, qkv_weight, preferred_element_type=f32)
        q_rot, k_rot, v_b, q_unit, k_unit, q_inv, k_inv = split_heads(packed, query_gain, key_gain, cosine, sine)
        attn_out, lse_blocks, starts = attend_forward(q_rot, k_rot, v_b, live)
        attn_flat = attn_out.reshape(group_rows, -1)
        middle = resid + block_sum([(attn_flat, out_weight)])
        inv_m = inv_rms(middle)
        unit_m = middle * inv_m
        normed_m = (unit_m * gain_m).astype(bf16)
        gate = jnp.dot(normed_m, gate_weight, preferred_element_type=f32)
        upper = jnp.dot(normed_m, up_weight, preferred_element_type=f32)
        sigma = jax.nn.sigmoid(gate)
        active = gate * sigma
        hidden = (active * upper).astype(bf16)
        block_out = middle + block_sum([(hidden, down_weight)])
        grad_b = grad_out.astype(bf16)
        d_down = jnp.dot(hidden.T, grad_b, preferred_element_type=f32)
        d_hidden = jnp.dot(grad_b, down_weight.T, preferred_element_type=f32)
        d_gate = (d_hidden * upper * sigma * (1.0 + gate * (1.0 - sigma))).astype(bf16)
        d_up = (d_hidden * active).astype(bf16)
        d_gatew = jnp.dot(normed_m.T, d_gate, preferred_element_type=f32)
        d_upw = jnp.dot(normed_m.T, d_up, preferred_element_type=f32)
        d_normed_m = block_sum([(d_gate, gate_weight.T), (d_up, up_weight.T)])
        mgain_part = lax.optimization_barrier(jnp.sum(d_normed_m * unit_m, axis=0))
        d_middle = grad_out + norm_back(d_normed_m * gain_m, unit_m, inv_m)
        d_middle_b = d_middle.astype(bf16)
        d_outw = jnp.dot(attn_flat.T, d_middle_b, preferred_element_type=f32)
        d_attn = jnp.dot(d_middle_b, out_weight.T, preferred_element_type=f32).astype(bf16).reshape(attn_out.shape)
        q_grad, k_grad, v_grad = attend_backward(q_rot, k_rot, v_b, live, lse_blocks, starts, d_attn)
        d_packed, qgain_part, kgain_part = merge_back(q_grad, k_grad, v_grad, q_unit, k_unit, q_inv, k_inv, query_gain, key_gain, cosine, sine)
        d_qkvw = jnp.dot(normed_a.T, d_packed, preferred_element_type=f32)
        d_normed_a = block_sum([(d_packed, qkv_weight.T)])
        again_part = lax.optimization_barrier(jnp.sum(d_normed_a * unit_a, axis=0))
        resid_grad = d_middle + norm_back(d_normed_a * gain_a, unit_a, inv_a)
        terms = (d_qkvw, d_outw, d_gatew, d_upw, d_down, again_part, mgain_part, qgain_part, kgain_part)
        carry = tuple((old + new for old, new in zip(carry, terms)))
        return (carry, (block_out, resid_grad))
    init = (jnp.zeros(qkv_weight.shape, f32), jnp.zeros(out_weight.shape, f32), jnp.zeros(gate_weight.shape, f32), jnp.zeros(up_weight.shape, f32), jnp.zeros(down_weight.shape, f32), jnp.zeros((width,), f32), jnp.zeros((width,), f32), jnp.zeros(query_gain.shape, f32), jnp.zeros(key_gain.shape, f32))
    items = (resid_in.reshape(groups, group_rows, width), lengths, out_grad.reshape(groups, group_rows, width))
    totals, (outputs, input_grads) = lax.scan(one_group, init, items)
    return (outputs.reshape(resid_in.shape), input_grads.reshape(resid_in.shape), totals[0], totals[1], totals[2], totals[3], totals[4], totals[5], totals[6], totals[7], totals[8])
```

```python
import functools

import jax
import jax.numpy as jnp
from jax import lax
from jax.experimental import pallas as pl
from jax.experimental.pallas import tpu as pltpu
from jax.sharding import PartitionSpec as P

HEADS = 32
KV_HEADS = 8
HEAD_DIM = 64
EPS = 1e-05
ROPE_BASE = 1000000.0
LANES = 2 * HEAD_DIM
PENALTY = 16384.0
F32 = jnp.float32
BF16 = jnp.bfloat16


def inv_rms(value):
    return lax.rsqrt(jnp.mean(value * value, axis=-1, keepdims=True) + EPS)


def norm_back(grad_unit, unit, inverse):
    return inverse * (grad_unit - unit * jnp.mean(grad_unit * unit, axis=-1, keepdims=True))


def lane_ids(rows):
    return lax.broadcasted_iota(jnp.int32, (rows, LANES), 1)


def head_mean_matrix():
    row = lax.broadcasted_iota(jnp.int32, (LANES, LANES), 0) // HEAD_DIM
    col = lax.broadcasted_iota(jnp.int32, (LANES, LANES), 1) // HEAD_DIM
    return jnp.where(row == col, 1.0, 0.0).astype(BF16)


def head_sum(value, ones):
    high = value.astype(BF16)
    low = (value - high.astype(F32)).astype(BF16)
    return jnp.dot(high, ones, preferred_element_type=F32) + jnp.dot(
        low, ones, preferred_element_type=F32
    )


def swap_halves(value, lane):
    half = HEAD_DIM // 2
    return jnp.where(
        (lane % HEAD_DIM) < half, pltpu.roll(value, LANES - half, 1), pltpu.roll(value, half, 1)
    )


def unit_of(value, ones):
    inverse = lax.rsqrt(head_sum(value * value, ones) * (1.0 / HEAD_DIM) + EPS)
    return value * inverse, inverse


def dot_t(left, right):
    return lax.dot_general(left, right, (((1,), (1,)), ((), ())), preferred_element_type=F32)


def causal(rows, keys_first):
    shape = (2 * rows, rows) if keys_first else (rows, 2 * rows)
    key = lax.broadcasted_iota(jnp.int32, shape, 0 if keys_first else 1) % rows
    query = lax.broadcasted_iota(jnp.int32, shape, 1 if keys_first else 0)
    return key <= query


def tensor_rows(block, rows, count):
    shift = lax.rem(block - lax.axis_index("tensor") + count, count)
    return pl.ds(pl.multiple_of(shift * rows, rows), rows)


def forward_kernel(
    blocks, hook, packed, cosine, sine, later, gains, attn, total, q_all, keys_all, values_all, acc
):
    rows = packed.shape[0] // blocks
    groups = packed.shape[1] // (3 * LANES)
    lane = lane_ids(rows)
    low = lane < HEAD_DIM
    ones = head_mean_matrix()
    zero = jnp.zeros((rows, LANES), BF16)
    scale = HEAD_DIM ** (-0.5)

    def prepare(block, carry):
        here = tensor_rows(block, rows, blocks)
        there = pl.ds(pl.multiple_of(block * rows, rows), rows)
        cos, sin = cosine[here, :], sine[here, :]
        second = later[here, :]
        pen = jnp.where(lane == 0, 1.0 - second, 0.0).astype(BF16)
        for group in range(groups):
            for tile in range(2):
                col = (3 * group + tile) * LANES
                unit, _ = unit_of(packed[here, col : col + LANES], ones)
                unit = unit * gains[0:1, :]
                turned = unit * cos + swap_halves(unit, lane) * sin
                q_all[there, (2 * group + tile) * LANES : (2 * group + tile + 1) * LANES] = (
                    turned * scale
                ).astype(BF16)
            col = (3 * group + 2) * LANES
            raw = packed[here, col : col + LANES]
            unit, _ = unit_of(raw, ones)
            unit = unit * gains[1:2, :]
            turned = unit * cos + swap_halves(unit, lane) * sin
            k_low = jnp.where(low, turned, 0.0)
            v_high = jnp.where(low, 0.0, raw)
            keys_all[group, block, 0:rows, 0:LANES] = k_low.astype(BF16)
            keys_all[group, block, rows : 2 * rows, 0:LANES] = pltpu.roll(
                k_low, HEAD_DIM, 1
            ).astype(BF16)
            keys_all[group, block, 0:rows, LANES : 2 * LANES] = pen
            keys_all[group, block, rows : 2 * rows, LANES : 2 * LANES] = pen
            values_all[group, block, 0:rows, 0:LANES] = pltpu.roll(v_high, HEAD_DIM, 1).astype(BF16)
            values_all[group, block, rows : 2 * rows, 0:LANES] = v_high.astype(BF16)
            values_all[group, block, 0:rows, LANES : 2 * LANES] = jnp.where(low, 1.0, 0.0).astype(
                BF16
            )
            values_all[group, block, rows : 2 * rows, LANES : 2 * LANES] = jnp.where(
                low, 0.0, 1.0
            ).astype(BF16)
        return carry

    lax.fori_loop(0, blocks, prepare, 0)

    def one_block(step, carry):
        tile, block = step // blocks, lax.rem(step, blocks)
        group = tile // 2
        here = tensor_rows(block, rows, blocks)
        there = pl.ds(pl.multiple_of(block * rows, rows), rows)
        cols = pl.ds(pl.multiple_of(tile * LANES, LANES), LANES)
        pen = jnp.where(lane == 0, -PENALTY * later[here, :], 0.0).astype(BF16)
        query = jnp.concatenate([q_all[there, cols], pen], axis=1)

        score = dot_t(query, keys_all[group, block])
        expo = jnp.where(causal(rows, False), jnp.exp(score), 0.0).astype(BF16)
        acc[...] = jnp.dot(expo, values_all[group, block], preferred_element_type=F32)

        def earlier(past, inner):
            expo = jnp.exp(dot_t(query, keys_all[group, past])).astype(BF16)
            acc[...] += jnp.dot(expo, values_all[group, past], preferred_element_type=F32)
            return inner

        lax.fori_loop(0, block, earlier, 0)
        amount = acc[:, LANES : 2 * LANES]
        attn[here, cols] = (acc[:, 0:LANES] / amount).astype(BF16)
        total[here, cols] = amount
        hook(step)
        return carry

    lax.fori_loop(0, 2 * groups * blocks, one_block, 0)


def vmem_specs(count):
    return [pl.BlockSpec(memory_space=pltpu.VMEM)] * count


def backward_kernel(
    blocks,
    packed,
    cosine,
    sine,
    later,
    gains,
    attn,
    total,
    q_all,
    keys_all,
    values_all,
    d_attn,
    d_packed,
    gain_parts,
    dq_acc,
    dk_acc,
    dv_acc,
):
    rows = packed.shape[0] // blocks
    groups = packed.shape[1] // (3 * LANES)
    lane = lane_ids(rows)
    low = lane < HEAD_DIM
    ones = head_mean_matrix()
    scale = HEAD_DIM ** (-0.5)
    gain_parts[...] = jnp.zeros_like(gain_parts)

    def turn_back(grad, here):
        return grad * cosine[here, :] - swap_halves(grad, lane) * sine[here, :]

    def norm_grad(turned, raw, gain):
        unit, inverse = unit_of(raw, ones)
        scaled = turned * gain
        mean = head_sum(scaled * unit, ones) * (1.0 / HEAD_DIM)
        part = jnp.sum((turned * unit).reshape(rows // 8, 8, LANES), axis=0)
        return inverse * (scaled - unit * mean), part

    def one_block(step, carry):
        tile, block = step // blocks, lax.rem(step, blocks)
        group = tile // 2
        here = tensor_rows(block, rows, blocks)
        there = pl.ds(pl.multiple_of(block * rows, rows), rows)
        cols = pl.ds(pl.multiple_of(tile * LANES, LANES), LANES)
        query = q_all[there, cols]
        pen = jnp.where(lane == 0, -PENALTY * later[here, :], 0.0).astype(BF16)
        query_wide = jnp.concatenate([query, pen], axis=1)
        grad = d_attn[here, cols].astype(F32)
        share = 1.0 / total[here, cols]
        delta = -head_sum(grad * attn[here, cols].astype(F32), ones) * share
        delta_high = delta.astype(BF16)
        delta_low = (delta - delta_high.astype(F32)).astype(BF16)
        place = lane % HEAD_DIM
        extra = jnp.where(
            place == 0, delta_high.astype(F32), jnp.where(place == 1, delta_low.astype(F32), 0.0)
        ).astype(BF16)
        grad_b = (grad * share).astype(BF16)
        grad_wide = jnp.concatenate([grad_b, extra], axis=1)

        def pair(past, diagonal, first):
            keys = keys_all[group, past]
            expo = jnp.exp(dot_t(keys, query_wide))
            if diagonal:
                expo = jnp.where(causal(rows, True), expo, 0.0)
            d_prob = dot_t(values_all[group, past], grad_wide)
            d_score = (expo * d_prob).astype(BF16)
            dk = jnp.dot(d_score, query, preferred_element_type=F32)
            dv = jnp.dot(expo.astype(BF16), grad_b, preferred_element_type=F32)
            dq = lax.dot_general(
                d_score,
                keys[:, 0:LANES],
                (((0,), (0,)), ((), ())),
                preferred_element_type=F32,
            )
            return dq, dk, dv

        dq, dk, dv = pair(block, True, True)
        dq_acc[...] = dq
        fresh = lax.rem(tile, 2) == 0

        @pl.when(fresh)
        def _():
            dk_acc[block] = dk
            dv_acc[block] = dv

        @pl.when(jnp.logical_not(fresh))
        def _():
            dk_acc[block] += dk
            dv_acc[block] += dv

        def earlier(past, inner):
            dq, dk, dv = pair(past, False, False)
            dq_acc[...] += dq
            dk_acc[past] += dk
            dv_acc[past] += dv
            return inner

        lax.fori_loop(0, block, earlier, 0)
        source = pl.ds(pl.multiple_of((group * 3 + lax.rem(tile, 2)) * LANES, LANES), LANES)
        turned = turn_back(dq_acc[...] * scale, here)
        out, part = norm_grad(turned, packed[here, source], gains[0:1, :])
        d_packed[here, source] = out.astype(BF16)
        gain_parts[0:8, :] += part

        @pl.when(jnp.logical_and(jnp.logical_not(fresh), block == blocks - 1))
        def _():
            source = pl.ds(pl.multiple_of((group * 3 + 2) * LANES, LANES), LANES)

            def finish(past, inner):
                here = tensor_rows(past, rows, blocks)
                dk = jnp.where(low, dk_acc[past, 0:rows, :], 0.0) + pltpu.roll(
                    jnp.where(low, 0.0, dk_acc[past, rows : 2 * rows, :]), HEAD_DIM, 1
                )
                dv = jnp.where(low, 0.0, dv_acc[past, rows : 2 * rows, :]) + pltpu.roll(
                    jnp.where(low, dv_acc[past, 0:rows, :], 0.0), HEAD_DIM, 1
                )
                turned = turn_back(dk, here)
                out, part = norm_grad(turned, packed[here, source], gains[1:2, :])
                d_packed[here, source] = jnp.where(low, out, dv).astype(BF16)
                gain_parts[8:16, :] += part
                return inner

            lax.fori_loop(0, blocks, finish, 0)

        return carry

    lax.fori_loop(0, 2 * groups * blocks, one_block, 0)


def attend_backward(blocks, packed, cosine, sine, later, gains, attn, total, saved, d_attn):
    height, width = packed.shape
    groups = width // (3 * LANES)
    rows = height // blocks
    return pl.pallas_call(
        functools.partial(backward_kernel, blocks),
        out_shape=(
            jax.ShapeDtypeStruct((height, width), BF16),
            jax.ShapeDtypeStruct((16, LANES), F32),
        ),
        in_specs=vmem_specs(11),
        out_specs=tuple(vmem_specs(2)),
        scratch_shapes=[
            pltpu.VMEM((rows, LANES), F32),
            pltpu.VMEM((blocks, 2 * rows, LANES), F32),
            pltpu.VMEM((blocks, 2 * rows, LANES), F32),
        ],
        cost_estimate=pl.CostEstimate(
            flops=20 * height * height * width, bytes_accessed=10 * height * width, transcendentals=0
        ),
        name="attend_backward",
    )(packed, cosine, sine, later, gains, attn, total, *saved, d_attn)


MESH = pl.DeviceIdType.MESH


class Place:
    def __init__(self, ring, chips):
        self.ring, self.chips = ring, chips
        self.dp, self.at = lax.axis_index("dp"), lax.axis_index("tensor")
        self.chip, self.core = self.dp // 2, lax.rem(self.dp, 2)

    def along(self, ahead):
        return (self.dp, lax.rem(self.at + ahead, self.ring))

    def chip_dp(self, ahead):
        return lax.rem(self.chip + ahead, self.chips) * 2 + self.core

    def partner(self):
        return (self.chip * 2 + 1 - self.core, self.at)

    def meet(self):
        peers = [self.along(k) for k in range(1, self.ring)]
        peers += [(self.chip_dp(k), self.at) for k in range(1, self.chips)] + [self.partner()]
        barrier = pltpu.get_barrier_semaphore()
        for peer in peers:
            pl.semaphore_signal(barrier, inc=1, device_id=peer, device_id_type=MESH)
        pl.semaphore_wait(barrier, len(peers))


def when(condition, action):
    if condition is None:
        action()
    else:
        pl.when(condition)(action)


class Send:
    def __init__(self, src, dst, sems, index, device, starts=None, lands=None):
        self.copy = pltpu.make_async_remote_copy(
            src_ref=src,
            dst_ref=dst,
            send_sem=sems[0].at[index],
            recv_sem=sems[1].at[index],
            device_id=device,
            device_id_type=MESH,
        )
        self.starts, self.lands = starts, lands

    def start(self):
        when(self.starts, self.copy.start)

    def landed(self):
        when(self.lands, self.copy.wait_recv)

    def sent(self):
        when(self.starts, self.copy.wait_send)


class LineGather:
    def __init__(self, place, block, slots, sems):
        n, at = place.ring, place.at
        above = (place.dp, jnp.minimum(at + 1, n - 1))
        below = (place.dp, jnp.maximum(at - 1, 0))
        self.steps = [None]
        for s in range(1, n):
            up_from = block if s == 1 else slots.at[n - s + 1]
            down_from = block if s == 1 else slots.at[s - 1]
            self.steps.append(
                (
                    Send(
                        up_from,
                        slots.at[n - s],
                        sems,
                        2 * (s - 1),
                        above,
                        (at >= s - 1) & (at < n - 1),
                        at >= s,
                    ),
                    Send(
                        down_from,
                        slots.at[s],
                        sems,
                        2 * (s - 1) + 1,
                        below,
                        (at >= 1) & (at + s <= n),
                        at + s < n,
                    ),
                )
            )

    @staticmethod
    def semaphores(ring):
        count = max(2 * (ring - 1), 1)
        return [pltpu.SemaphoreType.DMA((count,)), pltpu.SemaphoreType.DMA((count,))]

    def begin(self):
        for send in self.steps[1]:
            send.start()

    def step(self, s):
        for send in self.steps[s]:
            send.landed()
        if s + 1 < len(self.steps):
            for send in self.steps[s + 1]:
                send.start()

    def end(self):
        for pair in self.steps[1:]:
            for send in pair:
                send.sent()


class Spread:
    def __init__(self, place, shard, full, sems):
        chips = place.chips
        partner_dp = place.partner()[0]
        self.direct, self.relay = [], []
        for k in range(1, chips):
            target = place.chip_dp(k)
            self.direct.append(
                Send(shard, full.at[place.dp], sems, k, (target, place.at))
            )
        for k in range(chips):
            origin = place.chip_dp(chips - k)
            source = shard if k == 0 else full.at[origin]
            self.relay.append(Send(source, full.at[origin], sems, chips + k, place.partner()))

    @staticmethod
    def semaphores(chips):
        return [pltpu.SemaphoreType.DMA((2 * chips,)), pltpu.SemaphoreType.DMA((2 * chips,))]

    def begin(self):
        for send in self.direct:
            send.start()
        self.relay[0].start()

    def pass_on(self, k):
        self.direct[k - 1].landed()
        self.relay[k].start()

    def end(self):
        for send in self.relay:
            send.landed()
        for send in self.direct + self.relay:
            send.sent()


class Swap:
    def __init__(self, place, parts, slots, sems):
        n = place.ring
        self.sends = [
            Send(parts(k), slots.at[n - k], sems, k - 1, place.along(k)) for k in range(1, n)
        ]

    semaphores = LineGather.semaphores

    def begin(self):
        for send in self.sends:
            send.start()

    def end(self):
        for send in self.sends:
            send.landed()
        for send in self.sends:
            send.sent()


def any_specs(count):
    return [pl.BlockSpec(memory_space=pl.ANY)] * count


def remote_params(ident, **more):
    return pltpu.CompilerParams(collective_id=ident, has_side_effects=True, **more)


def gather_kernel(ring, chips, block, shard, slots, full, zs, zr, ws, wr, local):
    place = Place(ring, chips)
    own = [
        pltpu.make_async_copy(block, slots.at[0], local.at[0]),
        pltpu.make_async_copy(shard, full.at[place.dp], local.at[1]),
    ]
    place.meet()
    rows = LineGather(place, block, slots, (zs, zr))
    weight = Spread(place, shard, full, (ws, wr))
    rows.begin()
    weight.begin()
    for copy in own:
        copy.start()
    for s in range(1, ring):
        rows.step(s)
    for k in range(1, chips):
        weight.pass_on(k)
    rows.end()
    weight.end()
    for copy in own:
        copy.wait()


def gather_rows(ring, chips, block, shard):
    return pl.pallas_call(
        functools.partial(gather_kernel, ring, chips),
        out_shape=(
            jax.ShapeDtypeStruct((ring,) + block.shape, block.dtype),
            jax.ShapeDtypeStruct((2 * chips,) + shard.shape, shard.dtype),
        ),
        in_specs=vmem_specs(2),
        out_specs=tuple(any_specs(2)),
        scratch_shapes=LineGather.semaphores(ring)
        + Spread.semaphores(chips)
        + [pltpu.SemaphoreType.DMA((2,))],
        compiler_params=remote_params(1),
        name="gather_rows",
    )(block, shard)


def attend_gather_kernel(
    ring, chips, packed, cosine, sine, later, gains, block, shard, attn_own, total, q_all, keys_all,
    values_all, attn, slots, full, acc, zs, zr, ws, wr, xs, xr, local,
):
    place = Place(ring, chips)
    rows = packed.shape[0] // ring
    steps = 2 * (packed.shape[1] // (3 * LANES)) * ring
    own = [
        pltpu.make_async_copy(block, slots.at[0], local.at[0]),
        pltpu.make_async_copy(shard, full.at[place.dp], local.at[1]),
    ]
    place.meet()
    grads = LineGather(place, block, slots, (zs, zr))
    weight = Spread(place, shard, full, (ws, wr))
    grads.begin()
    weight.begin()
    for copy in own:
        copy.start()

    def hook(step):
        pl.when(step == (5 * steps) // 8)(lambda: grads.step(1))

    forward_kernel(
        ring, hook, packed, cosine, sine, later, gains, attn, total, q_all, keys_all, values_all, acc
    )
    swap = Swap(place, lambda k: attn.at[pl.ds(k * rows, rows)], attn_own, (xs, xr))
    swap.begin()
    kept = pltpu.make_async_copy(attn.at[pl.ds(0, rows)], attn_own.at[0], local.at[2])
    kept.start()
    for s in range(2, ring):
        if s - 1 < chips:
            weight.pass_on(s - 1)
        grads.step(s)
    for k in range(max(ring - 1, 1), chips):
        weight.pass_on(k)
    swap.end()
    grads.end()
    weight.end()
    for copy in own + [kept]:
        copy.wait()


def attend_gather(ring, chips, packed, cosine, sine, later, gains, block, shard):
    height, width = packed.shape
    groups = width // (3 * LANES)
    rows = height // ring
    wide = 2 * groups * LANES
    return pl.pallas_call(
        functools.partial(attend_gather_kernel, ring, chips),
        out_shape=(
            jax.ShapeDtypeStruct((ring, rows, wide), BF16),
            jax.ShapeDtypeStruct((height, wide), F32),
            jax.ShapeDtypeStruct((height, wide), BF16),
            jax.ShapeDtypeStruct((groups, ring, 2 * rows, 2 * LANES), BF16),
            jax.ShapeDtypeStruct((groups, ring, 2 * rows, 2 * LANES), BF16),
            jax.ShapeDtypeStruct((height, wide), BF16),
            jax.ShapeDtypeStruct((ring,) + block.shape, block.dtype),
            jax.ShapeDtypeStruct((2 * chips,) + shard.shape, shard.dtype),
        ),
        in_specs=vmem_specs(7),
        out_specs=tuple(any_specs(1) + vmem_specs(5) + any_specs(2)),
        scratch_shapes=[pltpu.VMEM((rows, 2 * LANES), F32)]
        + LineGather.semaphores(ring)
        + Spread.semaphores(chips)
        + Swap.semaphores(ring)
        + [pltpu.SemaphoreType.DMA((3,))],
        compiler_params=remote_params(2),
        name="attend_gather",
    )(packed, cosine, sine, later, gains, block, shard)


def hidden_kernel(
    ring, chips, block, shard, gate_hbm, up_hbm, slots, gate_out, up_out, full, gate_w, up_w, gate_v,
    up_v, zs, zr, ws, wr, local, load, put,
):
    place = Place(ring, chips)
    rows = block.shape[0]
    wide = gate_w.shape[1]
    tile = min(512, wide)
    own = [
        pltpu.make_async_copy(block, slots.at[0], local.at[0]),
        pltpu.make_async_copy(shard, full.at[place.dp], local.at[1]),
    ]
    loads = [
        pltpu.make_async_copy(gate_hbm, gate_w, load.at[0]),
        pltpu.make_async_copy(up_hbm, up_w, load.at[1]),
    ]
    for copy in loads:
        copy.start()
    place.meet()
    normed = LineGather(place, block, slots, (zs, zr))
    weight = Spread(place, shard, full, (ws, wr))
    normed.begin()
    weight.begin()
    for copy in own:
        copy.start()

    def puts(buffer, slot):
        here = pl.ds(slot * rows, rows)
        return [
            pltpu.make_async_copy(gate_v.at[buffer], gate_out.at[here], put.at[buffer, 0]),
            pltpu.make_async_copy(up_v.at[buffer], up_out.at[here], put.at[buffer, 1]),
        ]

    def multiply(buffer, slot, source, condition):
        def run():
            def one(index, carry):
                cols = pl.ds(pl.multiple_of(index * tile, tile), tile)
                left = source[...]
                gate_v[buffer, :, cols] = jnp.dot(
                    left, gate_w[:, cols], preferred_element_type=F32
                )
                up_v[buffer, :, cols] = jnp.dot(left, up_w[:, cols], preferred_element_type=F32)
                return carry

            lax.fori_loop(0, wide // tile, one, 0)
            for copy in puts(buffer, slot):
                copy.start()

        when(condition, run)

    def drain(buffer, slot, condition):
        def run():
            for copy in puts(buffer, slot):
                copy.wait()

        when(condition, run)

    for copy in loads:
        copy.wait()
    multiply(0, 0, block, None)
    drain(0, 0, None)
    at = place.at
    for s in range(1, ring):
        normed.step(s)
        if s < chips:
            weight.pass_on(s)
        came = [(s, at + s < ring), (ring - s, at >= s)]
        for buffer, (slot, condition) in enumerate(came):
            multiply(buffer, slot, slots.at[slot], condition)
        for buffer, (slot, condition) in enumerate(came):
            drain(buffer, slot, condition)
    for k in range(ring, chips):
        weight.pass_on(k)
    normed.end()
    weight.end()
    for copy in own:
        copy.wait()


def gather_hidden(ring, chips, block, shard, gate_full, up_full):
    rows, depth = block.shape
    wide = gate_full.shape[1]
    return pl.pallas_call(
        functools.partial(hidden_kernel, ring, chips),
        out_shape=(
            jax.ShapeDtypeStruct((ring, rows, depth), block.dtype),
            jax.ShapeDtypeStruct((ring * rows, wide), F32),
            jax.ShapeDtypeStruct((ring * rows, wide), F32),
            jax.ShapeDtypeStruct((2 * chips,) + shard.shape, shard.dtype),
        ),
        in_specs=vmem_specs(2) + any_specs(2),
        out_specs=tuple(vmem_specs(1) + any_specs(3)),
        scratch_shapes=[
            pltpu.VMEM(gate_full.shape, gate_full.dtype),
            pltpu.VMEM(up_full.shape, up_full.dtype),
            pltpu.VMEM((2, rows, wide), F32),
            pltpu.VMEM((2, rows, wide), F32),
        ]
        + LineGather.semaphores(ring)
        + Spread.semaphores(chips)
        + [
            pltpu.SemaphoreType.DMA((2,)),
            pltpu.SemaphoreType.DMA((2,)),
            pltpu.SemaphoreType.DMA((2, 2)),
        ],
        compiler_params=remote_params(3),
        name="gather_hidden",
    )(block, shard, gate_full, up_full)


def gather_line(block, axis, count):
    up, down = [block], [block]
    for step in range(1, count):
        up.append(lax.ppermute(up[-1], axis, [(i, i + 1) for i in range(step - 1, count - 1)]))
        down.append(lax.ppermute(down[-1], axis, [(i + 1, i) for i in range(0, count - step)]))
    return [block] + [
        pick(axis, slot, count, down[slot], up[count - slot]) for slot in range(1, count)
    ]


def pick(axis, slot, count, from_down, from_up):
    return jnp.where(lax.axis_index(axis) + slot < count, from_down, from_up)


def scatter_line(parts, axis, count):
    up, down = None, None
    for step in range(1, count):
        first, second = parts[count - step], parts[step]
        up = first if up is None else (first.astype(F32) + up.astype(F32)).astype(BF16)
        down = second if down is None else (second.astype(F32) + down.astype(F32)).astype(BF16)
        up = lax.ppermute(up, axis, [(i, i + 1) for i in range(0, step)])
        down = lax.ppermute(down, axis, [(i, i - 1) for i in range(count - step, count)])
    return parts[0].astype(F32) + up.astype(F32) + down.astype(F32)


def exchange(parts, axis, count):
    got = [parts[0]]
    for slot in range(1, count):
        pairs = [((i + slot) % count, i) for i in range(count)]
        got.append(lax.ppermute(parts[count - slot], axis, pairs))
    return got


def chip_groups(count):
    return [list(range(core, count, 2)) for core in range(2)]


def partner(count):
    return [(i, i ^ 1) for i in range(count)]


def by_core(value, axis, count):
    core = lax.rem(lax.axis_index("dp"), 2)
    shape = value.shape
    size = shape[axis] // count
    split = value.reshape(shape[:axis] + (count // 2, 2, size) + shape[axis + 1 :])
    out = []
    for which in (core, 1 - core):
        part = lax.dynamic_index_in_dim(split, which, axis + 1, keepdims=False)
        out.append(part.reshape(shape[:axis] + (shape[axis] // 2,) + shape[axis + 1 :]))
    return out


def weight_grad(rows_side, cols_side, axis, count):
    sides = [rows_side, cols_side]
    mine, other = by_core(sides[axis], 1, count)

    def product(part):
        pair = (part, cols_side) if axis == 0 else (rows_side, part)
        return jnp.dot(pair[0].T, pair[1], preferred_element_type=F32)

    sent = lax.ppermute(product(other).astype(BF16), "dp", partner(count))
    summed = (product(mine) + sent.astype(F32)).astype(BF16)
    return lax.psum_scatter(
        summed, "dp", scatter_dimension=axis, axis_index_groups=chip_groups(count), tiled=True
    ).astype(F32)


def per_device(
    resid_in,
    lengths,
    qkv_weight,
    out_weight,
    gate_weight,
    up_weight,
    down_weight,
    attn_gain,
    mlp_gain,
    query_gain,
    key_gain,
    out_grad,
):
    rows = resid_in.shape[0]
    ring = lax.axis_size("tensor")
    n_dp = lax.axis_size("dp")
    here = lax.axis_index("tensor")
    height = rows * ring

    gain_a = lax.all_gather(attn_gain, "dp", axis=0, tiled=True).astype(F32)
    inv_a = inv_rms(resid_in)
    unit_a = resid_in * inv_a
    normed_a = (unit_a * gain_a).astype(BF16)
    chips = n_dp // 2
    normed_a_all, gate_full = gather_rows(ring, chips, normed_a, gate_weight)
    normed_a_all = normed_a_all.reshape(height, -1)
    gate_full = gate_full.reshape(-1, gate_weight.shape[1])
    qkv_full = lax.all_gather(qkv_weight, "dp", axis=0, tiled=True)
    packed = jnp.dot(normed_a_all, qkv_full, preferred_element_type=F32)

    seq_length = lengths[0]
    spot = jnp.arange(height, dtype=jnp.int32)
    spot = lax.rem(spot // rows + here, ring) * rows + lax.rem(spot, rows)
    in_second = spot >= seq_length
    position = jnp.where(in_second, spot - seq_length, spot).astype(F32)
    half = HEAD_DIM // 2
    column = jnp.arange(LANES, dtype=jnp.int32)
    freq = ROPE_BASE ** (-(2.0 * lax.rem(column, half).astype(F32)) / HEAD_DIM)
    angle = position[:, None] * freq[None, :]
    cosine = jnp.cos(angle)
    sine = jnp.sin(angle) * jnp.where(lax.rem(column, HEAD_DIM) < half, -1.0, 1.0)[None, :]
    later = jnp.broadcast_to(in_second.astype(F32)[:, None], (height, LANES))
    gains = jnp.zeros((8, LANES), F32)
    gains = gains.at[0].set(jnp.concatenate([query_gain, query_gain]))
    gains = gains.at[1].set(jnp.concatenate([key_gain, jnp.zeros_like(key_gain)]))

    attn_own, total, *saved, attn, grad_all, up_full = attend_gather(
        ring, chips, packed, cosine, sine, later, gains, out_grad.astype(BF16), up_weight
    )
    grad_all = grad_all.reshape(height, -1)
    up_full = up_full.reshape(-1, up_weight.shape[1])
    attn_own = jnp.roll(attn_own, here, axis=0)
    attn_own = jnp.concatenate([attn_own[k] for k in range(ring)], axis=1)

    out_rows = lax.all_gather(out_weight, "tensor", axis=0, tiled=True)
    out_full = lax.all_gather(out_rows, "dp", axis=1, tiled=True)
    middle = resid_in + jnp.dot(attn_own, out_full, preferred_element_type=F32)

    gain_m = lax.all_gather(mlp_gain, "dp", axis=0, tiled=True).astype(F32)
    inv_m = inv_rms(middle)
    unit_m = middle * inv_m
    normed_m = (unit_m * gain_m).astype(BF16)
    normed_m_all, gate, upper, down_full = gather_hidden(
        ring, chips, normed_m, down_weight, gate_full, up_full
    )
    normed_m_all = normed_m_all.reshape(height, -1)
    down_full = down_full.transpose(1, 0, 2).reshape(down_weight.shape[0], -1)
    sigma = jax.nn.sigmoid(gate)
    active = gate * sigma
    hidden = (active * upper).astype(BF16)

    d_hidden = jnp.dot(grad_all, down_full.T, preferred_element_type=F32)
    d_gate = (d_hidden * upper * sigma * (1.0 + gate * (1.0 - sigma))).astype(BF16)
    d_up = (d_hidden * active).astype(BF16)
    d_norm_part = (
        jnp.dot(d_gate, gate_full.T, preferred_element_type=F32)
        + jnp.dot(d_up, up_full.T, preferred_element_type=F32)
    ).astype(BF16)
    d_normed_m = scatter_line(
        [d_norm_part[k * rows : (k + 1) * rows] for k in range(ring)], "tensor", ring
    )
    d_middle = out_grad + norm_back(d_normed_m * gain_m, unit_m, inv_m)
    d_middle_b = d_middle.astype(BF16)

    d_attn_own = jnp.dot(d_middle_b, out_full.T, preferred_element_type=F32).astype(BF16)
    wide = out_weight.shape[0]
    d_attn = jnp.concatenate(
        exchange(
            [
                lax.dynamic_slice_in_dim(d_attn_own, lax.rem(here + k, ring) * wide, wide, 1)
                for k in range(ring)
            ],
            "tensor",
            ring,
        ),
        axis=0,
    )
    d_packed, gain_parts = attend_backward(
        ring, packed, cosine, sine, later, gains, attn, total, saved, d_attn
    )
    d_norm_part = jnp.dot(d_packed, qkv_full.T, preferred_element_type=F32).astype(BF16)
    d_normed_a = scatter_line(
        [d_norm_part[k * rows : (k + 1) * rows] for k in range(ring)], "tensor", ring
    )
    resid_grad = d_middle + norm_back(d_normed_a * gain_a, unit_a, inv_a)

    mlp_part = jnp.dot(hidden, down_full, preferred_element_type=F32).astype(BF16)
    block_out = middle + scatter_line(
        [mlp_part[k * rows : (k + 1) * rows] for k in range(ring)], "tensor", ring
    )

    gate_grad = weight_grad(normed_m_all, d_gate, 0, n_dp)
    up_grad = weight_grad(normed_m_all, d_up, 0, n_dp)
    down_grad = weight_grad(hidden, grad_all, 1, n_dp)
    qkv_grad = weight_grad(normed_a_all, d_packed, 0, n_dp)
    out_part = weight_grad(attn_own, d_middle_b, 1, n_dp)
    outproj_grad = scatter_line(
        [
            lax.dynamic_slice_in_dim(out_part, lax.rem(here + k, ring) * wide, wide, 0).astype(BF16)
            for k in range(ring)
        ],
        "tensor",
        ring,
    )

    gain_sum_a = jnp.sum(qkv_weight.astype(F32) * qkv_grad, axis=1)
    gain_sum_m = jnp.sum(
        gate_weight.astype(F32) * gate_grad + up_weight.astype(F32) * up_grad, axis=1
    )
    gain_sums = lax.psum(jnp.stack([gain_sum_a, gain_sum_m]), "tensor")
    attngain_grad = gain_sums[0] / attn_gain.astype(F32)
    mlpgain_grad = gain_sums[1] / mlp_gain.astype(F32)
    small = lax.psum(jnp.sum(gain_parts.reshape(2, 8, LANES), axis=1), ("dp", "tensor"))
    querygain_grad = small[0, :HEAD_DIM] + small[0, HEAD_DIM:]
    keygain_grad = small[1, :HEAD_DIM]
    return (
        block_out,
        resid_grad,
        qkv_grad,
        outproj_grad,
        gate_grad,
        up_grad,
        down_grad,
        attngain_grad,
        mlpgain_grad,
        querygain_grad,
        keygain_grad,
    )


def solution(mesh):
    rows, weight = P(("dp", "tensor"), None), P("dp", "tensor")
    flipped, split = P("tensor", "dp"), P("dp")
    return jax.shard_map(
        per_device,
        mesh=mesh,
        in_specs=(
            rows,
            split,
            weight,
            flipped,
            weight,
            weight,
            flipped,
            split,
            split,
            P(),
            P(),
            rows,
        ),
        out_specs=(rows, rows, weight, flipped, weight, weight, flipped, split, split, P(), P()),
        check_vma=False,
    )
```
